256 devices in a mesh: row: 8 (over z), col: 32 (over y, x, core).
Axes of the slice: x: 4, y: 4, z: 8, core: 2. Of those that a mesh axis runs over, the one named last changes fastest.
Arguments:
- signs: int32 [1, 4096, 4096], P(None, 'row', 'col'), may hold values from 0 to 1
- upper_a: bfloat16 [4096, 4096], P('row'), may hold values from -1 to 1, as said below
- upper_b: bfloat16 [4096, 4096], P(None, 'col'), may hold values from -1 to 1, as said below
- diag_inverse: bfloat16 [4096, 512], P('row'), may hold values from -5 to 5
Outputs:
- solved: bfloat16 [1, 4096, 4096], P(None, 'row', 'col')
- col_norms: float32 [1, 4096], P(None, 'col')
- row_peaks: float32 [1, 4096], P(None, 'row')
The draws below stay inside these ranges and needn't reach their ends.
Inputs may be any that keep to these rules, and one draw needn't show every extreme that they name: `upper_a`: zero in every block of 512 x 512 on or below the block diagonal. `upper_b`: zero below its diagonal blocks of 128 x 128.
All inputs are finite; a program needn't handle non-finite values.
Results may differ from the reference program's by a relative error of at most 0.024.
Values may be sent and summed in bfloat16 or wider, within the bound.
A program may use at most 64 MiB of HBM per device.

```python
import math
import jax
import jax.numpy as jnp
from jax import lax

ORDER = 4096
PROBES = 1
SWEEPS = 3
BLKR = 512
BLKC = 128
N_ROW = 8
N_COL = 32


def draw_upper_a(key, part):
    block_id = jnp.arange(ORDER) // BLKR
    keep_mask = block_id[:, None] < block_id[None, :]
    spread_a = 0.4 / math.sqrt(ORDER)
    values = jnp.clip(jax.random.normal(key, (ORDER, ORDER), jnp.float32), -4.0, 4.0) * spread_a
    return jnp.where(keep_mask, values, 0.0).astype(jnp.bfloat16)


def draw_upper_b(key, part):
    block_id = jnp.arange(ORDER) // BLKC
    above_mask = block_id[:, None] < block_id[None, :]
    diag_mask = block_id[:, None] == block_id[None, :]
    spread_off = 0.4 / math.sqrt(ORDER)
    spread_diag = 0.2 / math.sqrt(BLKC)
    values = jnp.clip(jax.random.normal(key, (ORDER, ORDER), jnp.float32), -4.0, 4.0)
    scaled = jnp.where(diag_mask, values * spread_diag, jnp.where(above_mask, values * spread_off, 0.0))
    return scaled.astype(jnp.bfloat16)


def draw_diag_inverse(key, part):
    level_key, noise_key = jax.random.split(jax.random.fold_in(key, 17))
    row_id = jnp.arange(ORDER)
    rise = (row_id // BLKR * BLKR).astype(jnp.float32) / max(ORDER - BLKR, 1)
    level = jnp.exp(jax.random.uniform(level_key, (ORDER,), jnp.float32, math.log(0.3), 0.0))
    identity = ((row_id % BLKR)[:, None] == jnp.arange(BLKR)[None, :]).astype(jnp.float32)
    spread_d = 0.3 / math.sqrt(BLKR)
    growth = jnp.power(3.0, rise)
    noise = jnp.clip(jax.random.normal(noise_key, (ORDER, BLKR), jnp.float32), -4.0, 4.0) * spread_d
    scale = level * growth
    return (scale[:, None] * (identity + noise)).astype(jnp.bfloat16)


def touch_ends(result, rng, smallest, high):
    spot = [jax.random.randint(jax.random.fold_in(rng, axis), (), 0, length) for axis, length in enumerate(result.shape)]
    widest = result.shape.index(max(result.shape))
    next_to = spot[:widest] + [(spot[widest] + 1) % result.shape[widest]] + spot[widest + 1:]
    return result.at[tuple(spot)].set(smallest).at[tuple(next_to)].set(high)


def setup_inputs(seed: int = 0) -> dict:
    arg_keys = jax.random.split(jax.random.key(seed), 5)
    signs = touch_ends(jax.random.randint(arg_keys[0], (PROBES, ORDER, ORDER), 0, 2), jax.random.fold_in(arg_keys[0], 1), 0, 1).astype(jnp.int32)
    upper_a = draw_upper_a(jax.random.fold_in(arg_keys[4], 71), 0)
    upper_b = draw_upper_b(jax.random.fold_in(arg_keys[4], 71), 0)
    diag_inverse = draw_diag_inverse(jax.random.fold_in(arg_keys[4], 71), 0)
    return dict(signs=signs, upper_a=upper_a, upper_b=upper_b, diag_inverse=diag_inverse)


def product(left, right):
    return jnp.dot(left.astype(jnp.float32), right.astype(jnp.float32), precision=lax.Precision.HIGHEST, preferred_element_type=jnp.float32)


def block_solve(inverse_block, diag_part, residual):
    estimate = product(inverse_block, residual.astype(jnp.bfloat16)).astype(jnp.bfloat16)
    for number in range(SWEEPS):
        remainder = residual - product(estimate, diag_part)
        estimate = product(inverse_block, remainder.astype(jnp.bfloat16)).astype(jnp.bfloat16)
    return estimate


def reference(signs, upper_a, upper_b, diag_inverse):
    blk_rows = ORDER // N_ROW
    blk_cols = ORDER // N_COL
    outputs = []
    for number in range(PROBES):
        targets = (2 * signs[number] - 1).astype(jnp.float32)
        strips = [None] * N_ROW
        for row_block in reversed(range(N_ROW)):
            first_row = row_block * blk_rows
            last_row = first_row + blk_rows
            residual = targets[first_row:last_row]
            if row_block < N_ROW - 1:
                lower_rows = jnp.concatenate(strips[row_block + 1:], axis=0)
                residual = residual - product(upper_a[first_row:last_row, last_row:], lower_rows)
            inverse_block = diag_inverse[first_row:last_row]

            def advance(row_strip, column, residual=residual, inverse_block=inverse_block):
                offset = (column * blk_cols).astype(jnp.int32)
                own_block = lax.dynamic_slice_in_dim(residual, offset, blk_cols, 1)
                coupling = lax.dynamic_slice_in_dim(upper_b, offset, blk_cols, 1)
                diag_part = lax.dynamic_slice_in_dim(coupling, offset, blk_cols, 0)
                solution = block_solve(inverse_block, diag_part, own_block - product(row_strip, coupling))
                return lax.dynamic_update_slice_in_dim(row_strip, solution.astype(row_strip.dtype), offset, 1), None

            row_strip, unused = lax.scan(advance, jnp.zeros((blk_rows, ORDER), jnp.bfloat16), jnp.arange(N_COL, dtype=jnp.int32))
            strips[row_block] = row_strip
        outputs.append(jnp.concatenate(strips, axis=0))
    solved = jnp.stack(outputs)
    magnitude = jnp.abs(solved.astype(jnp.float32))
    return solved, jnp.sum(magnitude, axis=1), jnp.max(magnitude, axis=2)
```

```python
import functools

import jax
import jax.numpy as jnp
from jax import lax
from jax.experimental import pallas as pl
from jax.experimental.pallas import tpu as pltpu
from jax.sharding import PartitionSpec as P

MESH = pl.DeviceIdType.MESH
GROUP = 8
SOLVER = 1
HELPER = 0
TERMS = 4
F32 = jnp.float32
BF16 = jnp.bfloat16


def dot(left, right):
    return jnp.dot(left, right, preferred_element_type=F32)


def kernel(
    n_row, n_col,
    signs_ref, a_ref, b_ref, d_ref,
    out_ref, norm_ref, peak_ref,
    powers, couple, series, strip, solved, below, partial, passed, total, residual,
    stage, peaks, norm_all, peak_all, final_out,
    total_own, lower, own, partial_out, series_out, sign_out, sign_in, final_in,
    near_send, near_recv, far_send, far_recv, series_send, series_recv,
    sign_send, sign_recv, partial_send, partial_recv, below_send, below_recv,
    passed_send, passed_recv, relay_send, own_send, own_recv, lower_send, lower_recv,
    skip_send, norm_send, norm_recv, peak_send, peak_recv, final_send, final_recv,
):
    r = lax.axis_index("row")
    c = lax.axis_index("col")
    g = c // GROUP
    pos = c % GROUP
    first = g * GROUP
    n_group = n_col // GROUP
    bc = b_ref.shape[1]
    br = d_ref.shape[0]
    wide = GROUP * bc
    is_solver = pos == SOLVER
    is_helper = pos != SOLVER
    has_extra = pos == HELPER
    last_row = n_row - 1
    last_group = n_group - 1
    barrier = pltpu.get_barrier_semaphore()

    def remote(src, dst, send, recv, row, col):
        return pltpu.make_async_remote_copy(
            src_ref=src, dst_ref=dst, send_sem=send, recv_sem=recv,
            device_id=(row, col), device_id_type=MESH,
        )

    def greet(row, col):
        pl.semaphore_signal(barrier, inc=1, device_id=(row, col), device_id_type=MESH)

    def cols(index):
        return pl.ds(pl.multiple_of(index * bc, bc), bc)

    def rows(index, size):
        return pl.ds(pl.multiple_of(index * size, size), size)

    @pl.when(is_solver)
    def _():
        couple[rows(g, wide), :] = jnp.zeros((wide, wide), BF16)
        for p in range(GROUP):
            if p != SOLVER:
                greet(r, first + p)
        for step in range(1, n_row):
            greet((r + step) % n_row, c)
        for step in range(1, n_group):
            greet(r, (c + step * GROUP) % n_col)

        sign_out[...] = (2 * signs_ref[...] - 1).astype(BF16)
        strip[...] = jnp.zeros(strip.shape, BF16)
        total[...] = jnp.zeros(total.shape, F32)
        peaks[...] = jnp.zeros(peaks.shape, F32)
        diag = d_ref[...]
        second = dot(diag, diag).astype(BF16)
        powers[:, 0:br] = diag
        powers[:, br:2 * br] = second
        powers[:, 2 * br:3 * br] = dot(second, diag).astype(BF16)
        powers[:, 3 * br:4 * br] = dot(second, second).astype(BF16)
        mine = b_ref[cols(c), :]
        square = dot(mine, mine).astype(BF16)
        series[SOLVER, :, 0:bc] = -mine
        series[SOLVER, :, bc:2 * bc] = square
        series[SOLVER, :, 2 * bc:3 * bc] = (-dot(square, mine)).astype(BF16)
        for kb in range(SOLVER):
            couple[cols(first + kb), SOLVER * bc:(SOLVER + 1) * bc] = b_ref[cols(first + kb), :]
        for block in range(last_group):
            @pl.when(block < g)
            def _():
                couple[block * wide:(block + 1) * wide, SOLVER * bc:(SOLVER + 1) * bc] = b_ref[block * wide:(block + 1) * wide, :]

        pl.semaphore_wait(barrier, GROUP - 1 + n_row - 1 + n_group - 1)
        sign_copy = remote(sign_out, sign_in, sign_send, sign_recv, r, first + HELPER)
        sign_copy.start()

        def pass_on(k):
            return remote(passed.at[k], passed.at[k], relay_send.at[k], passed_recv.at[k], r, c + GROUP)

        for block in range(last_group):
            @pl.when(block < g)
            def _():
                for j in range(GROUP):
                    if j != SOLVER:
                        remote(
                            b_ref.at[pl.ds(block * wide, wide), :],
                            couple.at[pl.ds(block * wide, wide), pl.ds(j * bc, bc)],
                            far_send.at[block], far_recv.at[j, block], r, first + j,
                        ).wait_recv()

                def take(i, carry):
                    k = block * GROUP + i
                    remote(passed.at[k], passed.at[k], relay_send.at[k], passed_recv.at[k], r, (c + n_col - GROUP) % n_col).wait_recv()

                    @pl.when(g < last_group)
                    def _():
                        pass_on(k).start()

                    total[...] -= dot(passed[k], couple[cols(k), :])
                    return carry

                lax.fori_loop(0, GROUP, take, 0)

        def send_up(j):
            return remote(solved.at[j], below.at[j], below_send.at[j], below_recv.at[j], (r + n_row - 1) % n_row, c)

        def send_right(j):
            return remote(solved.at[j], passed.at[first + j], passed_send.at[j], passed_recv.at[first + j], r, (c + GROUP) % n_col)

        def send_own(j):
            return remote(solved.at[j], own.at[1], own_send.at[j], own_recv.at[1], r, first + j)

        def send_extra(j):
            return remote(solved.at[j], own.at[0], own_send.at[j], own_recv.at[0], r, first + HELPER)

        def column(j, carry):
            @pl.when(j != SOLVER)
            def _():
                remote(series_out, series.at[j], series_send, series_recv.at[j], r, first + j).wait_recv()
                for kb in range(GROUP - 1):
                    @pl.when(kb < j)
                    def _():
                        remote(
                            b_ref.at[cols(first + kb), :], couple.at[cols(first + kb), cols(j)],
                            near_send.at[kb], near_recv.at[j, kb], r, first + j,
                        ).wait_recv()

            near = dot(strip[...], couple[rows(g, wide), cols(j)])
            residual[...] = total[:, cols(j)] - near
            remote(partial_out.at[0], partial.at[j], partial_send.at[0], partial_recv.at[j], r, first + HELPER).wait_recv()
            residual[...] += partial[j].astype(F32)

            @pl.when(r < last_row)
            def _():
                send_down = remote(solved.at[j], below.at[j], below_send.at[j], below_recv.at[j], (r + 1) % n_row, c)
                send_down.wait_recv()
                residual[...] -= dot(a_ref[:, rows(r + 1, br)], below[j])

            lead = residual[...].astype(BF16)
            rest = dot(lead, series[j]).astype(BF16)
            stage[0:br, :] = lead
            for m in range(1, TERMS):
                stage[m * br:(m + 1) * br, :] = rest[:, (m - 1) * bc:m * bc]
            value = dot(powers[...], stage[...]).astype(BF16)
            solved[j] = value

            @pl.when(r > 0)
            def _():
                send_up(j).start()

            @pl.when(g < last_group)
            def _():
                send_right(j).start()

            @pl.when(j != SOLVER)
            def _():
                send_own(j).start()

            @pl.when(j == SOLVER)
            def _():
                send_extra(j).start()

            strip[:, cols(j)] = value
            magnitude = jnp.abs(value.astype(F32))
            peaks[...] = jnp.maximum(peaks[...], magnitude)
            norm_all[r, pl.ds(j, 1), :] = jnp.sum(magnitude, axis=0, keepdims=True)
            return carry

        lax.fori_loop(0, GROUP, column, 0)

        peak_all[g] = jnp.max(jnp.transpose(peaks[...]), axis=0, keepdims=True)
        for step in range(1, n_row):
            remote(norm_all.at[r], norm_all.at[r], norm_send.at[step - 1], norm_recv.at[r], (r + step) % n_row, c).start()
        for step in range(1, n_group):
            remote(peak_all.at[g], peak_all.at[g], peak_send.at[step - 1], peak_recv.at[g], r, (c + step * GROUP) % n_col).start()
        out_ref[...] = solved[SOLVER]
        for step in range(1, n_row):
            source = (r + step) % n_row
            remote(norm_all.at[source], norm_all.at[source], norm_send.at[step - 1], norm_recv.at[source], source, c).wait_recv()
        for step in range(1, n_group):
            source = (g + step) % n_group
            remote(peak_all.at[source], peak_all.at[source], peak_send.at[step - 1], peak_recv.at[source], r, source * GROUP + SOLVER).wait_recv()
        norms = norm_all[0]
        for source in range(1, n_row):
            norms = norms + norm_all[source]
        top = peak_all[0]
        for source in range(1, n_group):
            top = jnp.maximum(top, peak_all[source])
        for j in range(GROUP):
            final_out[j, :, 0:bc] = norms[j:j + 1, :]
            final_out[j, :, bc:bc + br] = top
        for j in range(GROUP):
            if j != SOLVER:
                remote(final_out.at[j], final_in, final_send.at[j], final_recv, r, first + j).start()
        norm_ref[...] = norms[SOLVER:SOLVER + 1, :]
        peak_ref[...] = top

        sign_copy.wait_send()
        for block in range(last_group):
            @pl.when((block < g) & (g < last_group))
            def _():
                def drain(i, carry):
                    pass_on(block * GROUP + i).wait_send()
                    return carry

                lax.fori_loop(0, GROUP, drain, 0)

        def finish(j, carry):
            @pl.when(r > 0)
            def _():
                send_up(j).wait_send()

            @pl.when(g < last_group)
            def _():
                send_right(j).wait_send()

            send_extra(j).wait_send()
            return carry

        lax.fori_loop(0, GROUP, finish, 0)
        for step in range(1, n_row):
            remote(norm_all.at[r], norm_all.at[r], norm_send.at[step - 1], norm_recv.at[r], (r + step) % n_row, c).wait_send()
        for step in range(1, n_group):
            remote(peak_all.at[g], peak_all.at[g], peak_send.at[step - 1], peak_recv.at[g], r, (c + step * GROUP) % n_col).wait_send()
        for j in range(GROUP):
            if j != SOLVER:
                remote(final_out.at[j], final_in, final_send.at[j], final_recv, r, first + j).wait_send()

    @pl.when(is_helper)
    def _():
        solver = first + SOLVER
        greet(r, solver)
        for step in (1, 2, n_row - 2, n_row - 1):
            greet((r + step) % n_row, c)
        mine = b_ref[cols(c), :]
        square = dot(mine, mine).astype(BF16)
        series_out[:, 0:bc] = -mine
        series_out[:, bc:2 * bc] = square
        series_out[:, 2 * bc:3 * bc] = (-dot(square, mine)).astype(BF16)
        total_own[1] = (2 * signs_ref[...] - 1).astype(F32)
        pl.semaphore_wait(barrier, 5)

        series_copy = remote(series_out, series.at[pos], series_send, series_recv.at[pos], r, solver)
        series_copy.start()

        def near_copy(kb):
            return remote(
                b_ref.at[cols(first + kb), :], couple.at[cols(first + kb), cols(pos)],
                near_send.at[kb], near_recv.at[pos, kb], r, solver,
            )

        def far_copy(block):
            return remote(
                b_ref.at[pl.ds(block * wide, wide), :],
                couple.at[pl.ds(block * wide, wide), cols(pos)],
                far_send.at[block], far_recv.at[pos, block], r, solver,
            )

        for kb in range(GROUP - 1):
            @pl.when(kb < pos)
            def _():
                near_copy(kb).start()
        for block in range(last_group):
            @pl.when(block < g)
            def _():
                far_copy(block).start()

        @pl.when(has_extra)
        def _():
            remote(sign_out, sign_in, sign_send, sign_recv, r, solver).wait_recv()
            total_own[0] = sign_in[...].astype(F32)

        def relay(slot, k):
            return remote(lower.at[slot, k], lower.at[slot, k], lower_send.at[slot, k], lower_recv.at[slot, k], (r + n_row - 1) % n_row, c)

        def apply(slot, k):
            remote(lower.at[slot, k], lower.at[slot, k], lower_send.at[slot, k], lower_recv.at[slot, k], (r + 1) % n_row, c).wait_recv()

            @pl.when(r > 0)
            def _():
                relay(slot, k).start()

            total_own[slot] -= dot(a_ref[:, rows(k, br)], lower[slot, k])

        def sweep(i, carry):
            k = last_row - i

            @pl.when(k >= r + 2)
            def _():
                apply(1, k)

                @pl.when(has_extra)
                def _():
                    apply(0, k)

            return carry

        lax.fori_loop(0, n_row - 2, sweep, 0)

        def give(slot, j):
            return remote(partial_out.at[slot], partial.at[j], partial_send.at[slot], partial_recv.at[j], r, solver)

        def skip(slot):
            return remote(own.at[slot], lower.at[slot, r], skip_send.at[slot], lower_recv.at[slot, r], (r + n_row - 2) % n_row, c)

        partial_out[1] = total_own[1].astype(BF16)
        give(1, pos).start()

        @pl.when(has_extra)
        def _():
            partial_out[0] = total_own[0].astype(BF16)
            give(0, SOLVER).start()

        remote(own.at[1], own.at[1], skip_send.at[1], own_recv.at[1], r, solver).wait_recv()

        @pl.when(r > 1)
        def _():
            skip(1).start()

        @pl.when(has_extra)
        def _():
            remote(own.at[0], own.at[0], skip_send.at[0], own_recv.at[0], r, solver).wait_recv()

            @pl.when(r > 1)
            def _():
                skip(0).start()

        out_ref[...] = own[1]

        series_copy.wait_send()
        for kb in range(GROUP - 1):
            @pl.when(kb < pos)
            def _():
                near_copy(kb).wait_send()
        for block in range(last_group):
            @pl.when(block < g)
            def _():
                far_copy(block).wait_send()
        give(1, pos).wait_send()

        @pl.when(has_extra)
        def _():
            give(0, SOLVER).wait_send()

        def settle(i, carry):
            k = last_row - i

            @pl.when((k >= r + 2) & (r > 0))
            def _():
                relay(1, k).wait_send()

                @pl.when(has_extra)
                def _():
                    relay(0, k).wait_send()

            return carry

        lax.fori_loop(0, n_row - 2, settle, 0)

        @pl.when(r > 1)
        def _():
            skip(1).wait_send()

            @pl.when(has_extra)
            def _():
                skip(0).wait_send()

        remote(final_in, final_in, final_send.at[0], final_recv, r, solver).wait_recv()
        norm_ref[...] = final_in[:, 0:bc]
        peak_ref[...] = final_in[:, bc:bc + br]


def solution(mesh):
    n_row = mesh.shape["row"]
    n_col = mesh.shape["col"]

    def shards(signs, upper_a, upper_b, diag_inverse):
        br = diag_inverse.shape[0]
        bc = upper_b.shape[1]
        order = upper_b.shape[0]
        wide = GROUP * bc
        n_group = n_col // GROUP
        dma = pltpu.SemaphoreType.DMA
        solved, norms, peaks = pl.pallas_call(
            functools.partial(kernel, n_row, n_col),
            out_shape=(
                jax.ShapeDtypeStruct((br, bc), BF16),
                jax.ShapeDtypeStruct((1, bc), F32),
                jax.ShapeDtypeStruct((1, br), F32),
            ),
            in_specs=[pl.BlockSpec(memory_space=pltpu.VMEM)] * 4,
            out_specs=[pl.BlockSpec(memory_space=pltpu.VMEM)] * 3,
            scratch_shapes=[
                pltpu.VMEM((br, TERMS * br), BF16),
                pltpu.VMEM((order, wide), BF16),
                pltpu.VMEM((GROUP, bc, (TERMS - 1) * bc), BF16),
                pltpu.VMEM((br, wide), BF16),
                pltpu.VMEM((GROUP, br, bc), BF16),
                pltpu.VMEM((GROUP, br, bc), BF16),
                pltpu.VMEM((GROUP, br, bc), BF16),
                pltpu.VMEM((n_col, br, bc), BF16),
                pltpu.VMEM((br, wide), F32),
                pltpu.VMEM((br, bc), F32),
                pltpu.VMEM((TERMS * br, bc), BF16),
                pltpu.VMEM((br, bc), F32),
                pltpu.VMEM((n_row, GROUP, bc), F32),
                pltpu.VMEM((n_group, 1, br), F32),
                pltpu.VMEM((GROUP, 1, bc + br), F32),
                pltpu.VMEM((2, br, bc), F32),
                pltpu.VMEM((2, n_row, br, bc), BF16),
                pltpu.VMEM((2, br, bc), BF16),
                pltpu.VMEM((2, br, bc), BF16),
                pltpu.VMEM((bc, (TERMS - 1) * bc), BF16),
                pltpu.VMEM((br, bc), BF16),
                pltpu.VMEM((br, bc), BF16),
                pltpu.VMEM((1, bc + br), F32),
                dma((GROUP,)), dma((GROUP, GROUP)),
                dma((n_group,)), dma((GROUP, n_group)),
                dma, dma((GROUP,)),
                dma, dma,
                dma((2,)), dma((GROUP,)),
                dma((GROUP,)), dma((GROUP,)),
                dma((GROUP,)), dma((n_col,)),
                dma((n_col,)),
                dma((GROUP,)), dma((2,)),
                dma((2, n_row)), dma((2, n_row)),
                dma((2,)),
                dma((n_row,)), dma((n_row,)),
                dma((n_group,)), dma((n_group,)),
                dma((GROUP,)), dma,
            ],
            compiler_params=pltpu.CompilerParams(
                collective_id=0, has_side_effects=True, vmem_limit_bytes=60 * 1024 * 1024
            ),
        )(signs[0], upper_a, upper_b, diag_inverse)
        return solved[None], norms, peaks

    in_specs = (P(None, "row", "col"), P("row", None), P(None, "col"), P("row", None))
    out_specs = (P(None, "row", "col"), P(None, "col"), P(None, "row"))
    return jax.shard_map(shards, mesh=mesh, in_specs=in_specs, out_specs=out_specs, check_vma=False)
```

```python
import functools

import jax
import jax.numpy as jnp
from jax import lax
from jax.experimental import pallas as pl
from jax.experimental.pallas import tpu as pltpu
from jax.sharding import PartitionSpec as P

MESH = pl.DeviceIdType.MESH
GROUP = 8
SOLVER = 1
SIDE = 0
PASS_FROM = 4
PASS_TO = 2
DOWN = 3
PARTS = 2
TERMS = 4
F32 = jnp.float32
BF16 = jnp.bfloat16


def dot(left, right):
    return jnp.dot(left, right, preferred_element_type=F32)


def kernel(
    n_row, n_col,
    signs_ref, a_ref, b_ref, d_ref,
    out_ref, norm_ref, peak_ref,
    powers, couple, series, strip, solved, below, partial, passed, total, residual,
    stage, peaks, norm_all, peak_all, final_out, next_a,
    total_own, lower, own, partial_out, sign_out, sign_in, final_in, all_a, bounce_near, bounce_far,
    near_send, near_recv, far_send, far_recv, copy_a,
    sign_send, sign_recv, partial_send, partial_recv, below_send, below_recv,
    passed_send, passed_recv, relay_send, own_send, own_recv, extra_send, down_send, up_send, lower_recv,
    skip_send, wrap_send, forward_send, bounce_send, bounce_recv, pass_send, norm_send, norm_recv, peak_send, peak_recv, final_send, final_recv,
):
    r = lax.axis_index("row")
    c = lax.axis_index("col")
    g = c // GROUP
    pos = c % GROUP
    first = g * GROUP
    n_group = n_col // GROUP
    bc = b_ref.shape[1]
    br = d_ref.shape[0]
    wide = GROUP * bc
    half = GROUP // 2
    chunk = br // PARTS
    last_row = n_row - 1
    last_group = n_group - 1
    solver = first + SOLVER
    barrier = pltpu.get_barrier_semaphore()

    def remote(src, dst, send, recv, row, col):
        return pltpu.make_async_remote_copy(
            src_ref=src, dst_ref=dst, send_sem=send, recv_sem=recv,
            device_id=(row, col), device_id_type=MESH,
        )

    def greet(row, col):
        pl.semaphore_signal(barrier, inc=1, device_id=(row, col), device_id_type=MESH)

    def cols(index):
        return pl.ds(pl.multiple_of(index * bc, bc), bc)

    def piece(h):
        return pl.ds(h * chunk, chunk)

    def rows(index, size):
        return pl.ds(pl.multiple_of(index * size, size), size)

    @pl.when(pos == SOLVER)
    def _():
        couple[rows(g, wide), :] = jnp.zeros((wide, wide), BF16)
        for p in range(GROUP):
            if p != SOLVER:
                greet(r, first + p)
        for step in range(1, n_row):
            greet((r + step) % n_row, c)
        for step in range(1, n_group):
            greet(r, (c + step * GROUP) % n_col)

        def fetch():
            return pltpu.make_async_copy(a_ref.at[:, rows(r + 1, br)], next_a, copy_a)

        @pl.when(r < last_row)
        def _():
            fetch().start()

        sign_out[...] = (2 * signs_ref[...] - 1).astype(BF16)
        strip[...] = jnp.zeros(strip.shape, BF16)
        total[...] = jnp.zeros(total.shape, F32)
        peaks[...] = jnp.zeros(peaks.shape, F32)
        for kb in range(SOLVER + 1):
            couple[cols(first + kb), SOLVER * bc:(SOLVER + 1) * bc] = b_ref[cols(first + kb), :]
        for block in range(last_group):
            @pl.when(block < g)
            def _():
                couple[block * wide:(block + 1) * wide, SOLVER * bc:(SOLVER + 1) * bc] = b_ref[block * wide:(block + 1) * wide, :]

        pl.semaphore_wait(barrier, GROUP - 1 + n_row - 1 + n_group - 1)

        def sign_copy():
            return remote(sign_out, sign_in.at[0], sign_send, sign_recv.at[0], r, first + half - 1)

        @pl.when(r < n_row - 2)
        def _():
            sign_copy().start()

        @pl.when(r >= n_row - 2)
        def _():
            partial[SOLVER] = sign_out[...]

        diag = d_ref[...]
        second = dot(diag, diag).astype(BF16)
        powers[:, 0:br] = diag
        powers[:, br:2 * br] = second
        powers[:, 2 * br:3 * br] = dot(second, diag).astype(BF16)
        powers[:, 3 * br:4 * br] = dot(second, second).astype(BF16)

        def pass_on(k):
            return remote(passed.at[k], passed.at[k], relay_send.at[k], passed_recv.at[k], r, (c + GROUP) % n_col)

        for block in range(last_group):
            @pl.when(block < g)
            def _():
                for j in range(GROUP):
                    if j != SOLVER:
                        remote(
                            b_ref.at[pl.ds(block * wide, wide), :],
                            couple.at[pl.ds(block * wide, wide), pl.ds(j * bc, bc)],
                            far_send.at[block], far_recv.at[j, block], r, first + j,
                        ).wait_recv()

                def take(i, carry):
                    k = block * GROUP + i
                    remote(passed.at[k], passed.at[k], relay_send.at[k], passed_recv.at[k], r, (c + n_col - GROUP) % n_col).wait_recv()

                    @pl.when(g < last_group)
                    def _():
                        pass_on(k).start()

                    total[...] -= dot(passed[k], couple[cols(k), :])
                    return carry

                lax.fori_loop(0, GROUP, take, 0)

        @pl.when(r < last_row)
        def _():
            fetch().wait()

        def send_up(j, h):
            return remote(solved.at[j, piece(h)], below.at[j, piece(h)], below_send.at[j, h], below_recv.at[j, h], (r + n_row - 1) % n_row, c)

        def send_right(j):
            return remote(solved.at[j], passed.at[first + j], passed_send.at[j], passed_recv.at[first + j], r, (c + GROUP) % n_col)

        def send_own(j, h):
            return remote(solved.at[j, piece(h)], own.at[1 + j % 2, piece(h)], own_send.at[j, h], own_recv.at[1 + j % 2, h], r, first + j // 2 * 2 + 1)

        def send_side(h):
            return remote(solved.at[SIDE, piece(h)], own.at[0, piece(h)], own_send.at[SIDE, h], own_recv.at[0, h], r, first)

        def send_extra(j, place, h):
            return remote(solved.at[j, piece(h)], own.at[0, piece(h)], extra_send.at[j, h], own_recv.at[0, h], r, first + place)

        def column(j, carry):
            @pl.when(j != SOLVER)
            def _():
                for kb in range(GROUP):
                    @pl.when(kb <= j)
                    def _():
                        remote(
                            b_ref.at[cols(first + kb), :], couple.at[cols(first + kb), cols(j)],
                            near_send.at[kb], near_recv.at[j, kb], r, first + j,
                        ).wait_recv()

            mine = couple[cols(first + j), cols(j)]
            square = dot(mine, mine).astype(BF16)
            series[:, 0:bc] = -mine
            series[:, bc:2 * bc] = square
            series[:, 2 * bc:3 * bc] = (-dot(square, mine)).astype(BF16)
            near = dot(strip[...], couple[rows(g, wide), cols(j)])
            residual[...] = total[:, cols(j)] - near

            @pl.when((j != SOLVER) | (r < n_row - 2))
            def _():
                remote(partial_out.at[1], partial.at[j], partial_send.at[1], partial_recv.at[j], r, first).wait_recv()

            residual[...] += partial[j].astype(F32)

            @pl.when(r < last_row)
            def _():
                for h in range(PARTS):
                    remote(
                        solved.at[j, piece(h)], below.at[j, piece(h)], below_send.at[j, h], below_recv.at[j, h], (r + 1) % n_row, c,
                    ).wait_recv()
                residual[...] -= dot(next_a[...], below[j])

            lead = residual[...].astype(BF16)
            rest = dot(lead, series[...]).astype(BF16)
            stage[0:br, :] = lead
            for m in range(1, TERMS):
                stage[m * br:(m + 1) * br, :] = rest[:, (m - 1) * bc:m * bc]
            for h in range(PARTS):
                solved[j, piece(h), :] = dot(powers[piece(h), :], stage[...]).astype(BF16)

                @pl.when(r > 0)
                def _():
                    send_up(j, h).start()

                @pl.when(r > 1)
                def _():
                    @pl.when(j == SIDE)
                    def _():
                        send_extra(SIDE, GROUP - 1, h).start()

                    @pl.when(j == SOLVER)
                    def _():
                        send_extra(SOLVER, half - 1, h).start()

                @pl.when(j > SOLVER)
                def _():
                    send_own(j, h).start()

                @pl.when(j == SIDE)
                def _():
                    send_side(h).start()

            @pl.when(g < last_group)
            def _():
                send_right(j).start()

            value = solved[j]
            strip[:, cols(j)] = value
            magnitude = jnp.abs(value.astype(F32))
            peaks[...] = jnp.maximum(peaks[...], magnitude)
            norm_all[r, pl.ds(j, 1), :] = jnp.sum(magnitude, axis=0, keepdims=True)
            return carry

        lax.fori_loop(0, GROUP, column, 0)

        peak_all[g] = jnp.max(jnp.transpose(peaks[...]), axis=0, keepdims=True)
        for step in range(1, n_row):
            remote(norm_all.at[r], norm_all.at[r], norm_send.at[step - 1], norm_recv.at[r], (r + step) % n_row, c).start()
        for step in range(1, n_group):
            remote(peak_all.at[g], peak_all.at[g], peak_send.at[step - 1], peak_recv.at[g], r, (c + step * GROUP) % n_col).start()
        out_ref[...] = solved[SOLVER]
        for step in range(1, n_row):
            source = (r + step) % n_row
            remote(norm_all.at[source], norm_all.at[source], norm_send.at[step - 1], norm_recv.at[source], source, c).wait_recv()
        for step in range(1, n_group):
            source = (g + step) % n_group
            remote(peak_all.at[source], peak_all.at[source], peak_send.at[step - 1], peak_recv.at[source], r, source * GROUP + SOLVER).wait_recv()
        norms = norm_all[0]
        for source in range(1, n_row):
            norms = norms + norm_all[source]
        top = peak_all[0]
        for source in range(1, n_group):
            top = jnp.maximum(top, peak_all[source])
        for j in range(GROUP):
            final_out[j, :, 0:bc] = norms[j:j + 1, :]
            final_out[j, :, bc:bc + br] = top
        for j in range(GROUP):
            if j != SOLVER:
                remote(final_out.at[j], final_in, final_send.at[j], final_recv, r, first + j).start()
        norm_ref[...] = norms[SOLVER:SOLVER + 1, :]
        peak_ref[...] = top

        @pl.when(r < n_row - 2)
        def _():
            sign_copy().wait_send()

        for block in range(last_group):
            @pl.when((block < g) & (g < last_group))
            def _():
                def drain(i, carry):
                    pass_on(block * GROUP + i).wait_send()
                    return carry

                lax.fori_loop(0, GROUP, drain, 0)

        def finish(j, carry):
            @pl.when(r > 0)
            def _():
                for h in range(PARTS):
                    send_up(j, h).wait_send()

            @pl.when(g < last_group)
            def _():
                send_right(j).wait_send()

            @pl.when(j > SOLVER)
            def _():
                for h in range(PARTS):
                    send_own(j, h).wait_send()

            return carry

        lax.fori_loop(0, GROUP, finish, 0)
        for h in range(PARTS):
            send_side(h).wait_send()

        @pl.when(r > 1)
        def _():
            for h in range(PARTS):
                send_extra(SIDE, GROUP - 1, h).wait_send()
                send_extra(SOLVER, half - 1, h).wait_send()

        for step in range(1, n_row):
            remote(norm_all.at[r], norm_all.at[r], norm_send.at[step - 1], norm_recv.at[r], (r + step) % n_row, c).wait_send()
        for step in range(1, n_group):
            remote(peak_all.at[g], peak_all.at[g], peak_send.at[step - 1], peak_recv.at[g], r, (c + step * GROUP) % n_col).wait_send()
        for j in range(GROUP):
            if j != SOLVER:
                remote(final_out.at[j], final_in, final_send.at[j], final_recv, r, first + j).wait_send()

    def near_copy(kb):
        return remote(
            b_ref.at[cols(first + kb), :], couple.at[cols(first + kb), cols(pos)],
            near_send.at[kb], near_recv.at[pos, kb], r, solver,
        )

    def far_copy(block):
        return remote(
            b_ref.at[pl.ds(block * wide, wide), :],
            couple.at[pl.ds(block * wide, wide), cols(pos)],
            far_send.at[block], far_recv.at[pos, block], r, solver,
        )

    def near_all():
        for kb in range(GROUP):
            @pl.when(kb <= pos)
            def _():
                near_copy(kb).start()

    def far_all():
        for block in range(last_group):
            @pl.when(block < g)
            def _():
                far_copy(block).start()

    def drain_all():
        for kb in range(GROUP):
            @pl.when(kb <= pos)
            def _():
                near_copy(kb).wait_send()
        for block in range(last_group):
            @pl.when(block < g)
            def _():
                far_copy(block).wait_send()

    def close():
        remote(final_in, final_in, final_send.at[0], final_recv, r, solver).wait_recv()
        norm_ref[...] = final_in[:, 0:bc]
        peak_ref[...] = final_in[:, bc:bc + br]

    def give(slot, j):
        return remote(partial_out.at[slot], partial.at[j], partial_send.at[slot], partial_recv.at[j], r, solver)

    def take_own(slot, h):
        remote(own.at[slot, piece(h)], own.at[slot, piece(h)], skip_send.at[0, h], own_recv.at[slot, h], r, solver).wait_recv()

    @pl.when(pos % 2 == 0)
    def _():
        greet(r, solver)

        @pl.when(pos == 0)
        def _():
            greet(r, first + GROUP - 1)

        @pl.when(pos > 0)
        def _():
            greet(r, c + 1)

        @pl.when(pos == PASS_FROM)
        def _():
            greet(r, first + PASS_TO)

        @pl.when(pos == PASS_TO)
        def _():
            greet(r, first + PASS_FROM)

        partial_out[1] = (2 * signs_ref[...] - 1).astype(BF16)

        @pl.when((pos == PASS_FROM) | (pos == PASS_TO))
        def _():
            pl.semaphore_wait(barrier, 3)

        @pl.when((pos != PASS_FROM) & (pos != PASS_TO))
        def _():
            pl.semaphore_wait(barrier, 2)

        def sign_zero():
            return remote(partial_out.at[1], sign_in.at[0], sign_send, sign_recv.at[0], r, first + GROUP - 1)

        def sign_next():
            return remote(partial_out.at[1], sign_in.at[1], sign_send, sign_recv.at[1], r, c + 1)

        def lend_near():
            return remote(b_ref.at[rows(g, wide), :], bounce_near, near_send.at[0], bounce_recv.at[n_group], r, first + PASS_TO)

        def lend_far(block):
            return remote(b_ref.at[pl.ds(block * wide, wide), :], bounce_far.at[block], far_send.at[block], bounce_recv.at[block], r, first + PASS_TO)

        def pass_near(kb):
            return remote(
                bounce_near.at[pl.ds(kb * bc, bc), :], couple.at[cols(first + kb), pl.ds(PASS_FROM * bc, bc)],
                bounce_send.at[kb], near_recv.at[PASS_FROM, kb], r, solver,
            )

        def pass_far(block):
            return remote(
                bounce_far.at[block], couple.at[pl.ds(block * wide, wide), pl.ds(PASS_FROM * bc, bc)],
                pass_send.at[block], far_recv.at[PASS_FROM, block], r, solver,
            )

        @pl.when((r < n_row - 2) & (pos == 0))
        def _():
            sign_zero().start()

        @pl.when((r < n_row - 2) & (pos > 0))
        def _():
            sign_next().start()

        @pl.when(pos != PASS_FROM)
        def _():
            far_all()

        for block in range(last_group):
            @pl.when((pos == PASS_FROM) & (block < g))
            def _():
                lend_far(block).start()

            @pl.when((pos == PASS_TO) & (block < g))
            def _():
                lend_far(block).wait_recv()
                pass_far(block).start()

        @pl.when(pos == PASS_FROM)
        def _():
            lend_near().start()

        @pl.when(pos != PASS_FROM)
        def _():
            near_all()

        @pl.when(r >= n_row - 2)
        def _():
            give(1, pos).start()

        @pl.when(pos == PASS_TO)
        def _():
            lend_near().wait_recv()
            for kb in range(PASS_FROM + 1):
                pass_near(kb).start()

        for h in range(PARTS):
            take_own(0, h)
        out_ref[...] = own[0]

        @pl.when(r < n_row - 2)
        def _():
            sign_next().wait_send()

        @pl.when(r >= n_row - 2)
        def _():
            give(1, pos).wait_send()

        @pl.when(pos == PASS_FROM)
        def _():
            lend_near().wait_send()
            for block in range(last_group):
                @pl.when(block < g)
                def _():
                    lend_far(block).wait_send()

        @pl.when(pos == PASS_TO)
        def _():
            for kb in range(PASS_FROM + 1):
                pass_near(kb).wait_send()
            for block in range(last_group):
                @pl.when(block < g)
                def _():
                    pass_far(block).wait_send()

        @pl.when(pos != PASS_FROM)
        def _():
            drain_all()

        close()

    @pl.when((pos % 2 == 1) & (pos > SOLVER))
    def _():
        upper = pos // half
        has_extra = pos % half == half - 1
        lag = upper

        def fetch():
            return pltpu.make_async_copy(a_ref, all_a, copy_a)

        greet(r, solver)
        greet(r, c - 1)
        for step in range(1, n_row):
            greet((r + step) % n_row, c)

        @pl.when(pos == GROUP - 1)
        def _():
            greet(r, first)

        fetch().start()
        signs = 2 * signs_ref[...] - 1
        total_own[2] = signs.astype(F32)
        partial_out[2] = signs.astype(BF16)

        @pl.when(pos == GROUP - 1)
        def _():
            pl.semaphore_wait(barrier, n_row + 2)

        @pl.when(pos < GROUP - 1)
        def _():
            pl.semaphore_wait(barrier, n_row + 1)

        far_all()
        near_all()

        @pl.when(r >= n_row - 2)
        def _():
            give(2, pos).start()


        @pl.when(r < n_row - 2)
        def _():
            remote(sign_in.at[1], sign_in.at[1], sign_send, sign_recv.at[1], r, c - 1).wait_recv()
            total_own[1] = sign_in[1].astype(F32)

            @pl.when(has_extra)
            def _():
                remote(sign_in.at[0], sign_in.at[0], sign_send, sign_recv.at[0], r, solver).wait_recv()
                total_own[0] = sign_in[0].astype(F32)

        fetch().wait()

        def lower_copy(slot, k, sems, row, h):
            return remote(lower.at[slot, k, piece(h)], lower.at[slot, k, piece(h)], sems.at[slot, k, h], lower_recv.at[slot, k, h], row, c)

        def relay_down(slot, k, h):
            return lower_copy(slot, k, down_send, (r + n_row - 1) % n_row, h)

        def relay_up(slot, k, h):
            return lower_copy(slot, k, up_send, (r + 1) % n_row, h)

        def skip(slot, h):
            return remote(own.at[slot, piece(h)], lower.at[slot, r, piece(h)], skip_send.at[slot, h], lower_recv.at[slot, r, h], (r + n_row - 2) % n_row, c)

        def wrap(slot, h):
            return remote(own.at[slot, piece(h)], lower.at[slot, r, piece(h)], wrap_send.at[slot, h], lower_recv.at[slot, r, h], 0, c)

        def forward(h):
            return remote(own.at[1, piece(h)], own.at[0, piece(h)], forward_send.at[h], own_recv.at[0, h], r, c - 1)

        def goes_down(k):
            return (k >= r + 2) & (k < r + DOWN) & (r > 0)

        def apply(slot, k):
            for h in range(PARTS):
                lower_copy(slot, k, down_send, (r + 1) % n_row, h).wait_recv()

                @pl.when(goes_down(k))
                def _():
                    relay_down(slot, k, h).start()

                @pl.when(k >= r + DOWN + 2)
                def _():
                    relay_up(slot, k, h).start()

            total_own[slot] -= dot(all_a[:, rows(k, br)], lower[slot, k])

        def handle(slot, k, j):
            @pl.when((k >= r + 2) & (k <= last_row))
            def _():
                apply(slot, k)

                @pl.when(k == r + 2)
                def _():
                    partial_out[slot] = total_own[slot].astype(BF16)
                    give(slot, j).start()

        def spread(slot):
            for h in range(PARTS):
                take_own(slot, h)

                @pl.when(r > 1)
                def _():
                    skip(slot, h).start()

                @pl.when(r > DOWN)
                def _():
                    wrap(slot, h).start()

        def event(i, carry):
            early = last_row - i
            late = last_row - i + lag

            @pl.when(has_extra)
            def _():
                handle(0, early, 1 - upper)

                @pl.when((early == r) & (r > 1))
                def _():
                    spread(0)

            handle(1, late, pos - 1)

            @pl.when(late == r)
            def _():
                spread(1)
                for h in range(PARTS):
                    forward(h).start()

            handle(2, late, pos)

            @pl.when(late == r)
            def _():
                spread(2)

            return carry

        lax.fori_loop(0, n_row + 2, event, 0)
        out_ref[...] = own[2]
        for h in range(PARTS):
            forward(h).wait_send()
        give(2, pos).wait_send()

        @pl.when(r < n_row - 2)
        def _():
            give(1, pos - 1).wait_send()

            @pl.when(has_extra)
            def _():
                give(0, 1 - upper).wait_send()

        def settle_slot(slot):
            def settle(i, carry):
                k = last_row - i

                @pl.when(goes_down(k))
                def _():
                    for h in range(PARTS):
                        relay_down(slot, k, h).wait_send()

                @pl.when(k >= r + DOWN + 2)
                def _():
                    for h in range(PARTS):
                        relay_up(slot, k, h).wait_send()

                return carry

            lax.fori_loop(0, n_row - 2, settle, 0)

            @pl.when(r > 1)
            def _():
                for h in range(PARTS):
                    skip(slot, h).wait_send()

            @pl.when(r > DOWN)
            def _():
                for h in range(PARTS):
                    wrap(slot, h).wait_send()

        @pl.when(has_extra)
        def _():
            settle_slot(0)

        settle_slot(1)
        settle_slot(2)
        drain_all()
        close()


def hand_out(solved_ref, norm_ref, peak_ref, solved_out, norm_out, peak_out):
    solved_out[...] = solved_ref[...]
    norm_out[...] = norm_ref[...]
    peak_out[...] = peak_ref[...]


def solution(mesh):
    n_row = mesh.shape["row"]
    n_col = mesh.shape["col"]

    def shards(signs, upper_a, upper_b, diag_inverse):
        br = diag_inverse.shape[0]
        bc = upper_b.shape[1]
        order = upper_b.shape[0]
        wide = GROUP * bc
        n_group = n_col // GROUP
        dma = pltpu.SemaphoreType.DMA
        vmem = pl.BlockSpec(memory_space=pltpu.VMEM)
        shapes = (
            jax.ShapeDtypeStruct((br, bc), BF16),
            jax.ShapeDtypeStruct((1, bc), F32),
            jax.ShapeDtypeStruct((1, br), F32),
        )
        results = pl.pallas_call(
            functools.partial(kernel, n_row, n_col),
            out_shape=shapes,
            in_specs=[vmem, pl.BlockSpec(memory_space=pl.ANY), vmem, vmem],
            out_specs=[vmem] * 3,
            scratch_shapes=[
                pltpu.VMEM((br, TERMS * br), BF16),
                pltpu.VMEM((order, wide), BF16),
                pltpu.VMEM((bc, (TERMS - 1) * bc), BF16),
                pltpu.VMEM((br, wide), BF16),
                pltpu.VMEM((GROUP, br, bc), BF16),
                pltpu.VMEM((GROUP, br, bc), BF16),
                pltpu.VMEM((GROUP, br, bc), BF16),
                pltpu.VMEM((n_col, br, bc), BF16),
                pltpu.VMEM((br, wide), F32),
                pltpu.VMEM((br, bc), F32),
                pltpu.VMEM((TERMS * br, bc), BF16),
                pltpu.VMEM((br, bc), F32),
                pltpu.VMEM((n_row, GROUP, bc), F32),
                pltpu.VMEM((n_group, 1, br), F32),
                pltpu.VMEM((GROUP, 1, bc + br), F32),
                pltpu.VMEM((br, br), BF16),
                pltpu.VMEM((3, br, bc), F32),
                pltpu.VMEM((3, n_row, br, bc), BF16),
                pltpu.VMEM((3, br, bc), BF16),
                pltpu.VMEM((3, br, bc), BF16),
                pltpu.VMEM((br, bc), BF16),
                pltpu.VMEM((2, br, bc), BF16),
                pltpu.VMEM((1, bc + br), F32),
                pltpu.VMEM((br, n_row * br), BF16),
                pltpu.VMEM((wide, bc), BF16),
                pltpu.VMEM((n_group, wide, bc), BF16),
                dma((GROUP,)), dma((GROUP, GROUP)),
                dma((n_group,)), dma((GROUP, n_group)),
                dma,
                dma, dma((2,)),
                dma((3,)), dma((GROUP,)),
                dma((GROUP, PARTS)), dma((GROUP, PARTS)),
                dma((GROUP,)), dma((n_col,)),
                dma((n_col,)),
                dma((GROUP, PARTS)), dma((3, PARTS)),
                dma((2, PARTS)),
                dma((3, n_row, PARTS)), dma((3, n_row, PARTS)), dma((3, n_row, PARTS)),
                dma((3, PARTS)), dma((3, PARTS)), dma((PARTS,)),
                dma((GROUP,)), dma((n_group + 1,)), dma((n_group,)),
                dma((n_row,)), dma((n_row,)),
                dma((n_group,)), dma((n_group,)),
                dma((GROUP,)), dma,
            ],
            compiler_params=pltpu.CompilerParams(
                collective_id=0, has_side_effects=True, vmem_limit_bytes=60 * 1024 * 1024
            ),
        )(signs[0], upper_a, upper_b, diag_inverse)
        solved, norms, peaks = pl.pallas_call(
            hand_out, out_shape=shapes, in_specs=[vmem] * 3, out_specs=[vmem] * 3
        )(*results)
        return solved[None], norms, peaks

    in_specs = (P(None, "row", "col"), P("row", None), P(None, "col"), P("row", None))
    out_specs = (P(None, "row", "col"), P(None, "col"), P(None, "row"))
    return jax.shard_map(shards, mesh=mesh, in_specs=in_specs, out_specs=out_specs, check_vma=False)
```

```python
import functools

import jax
import jax.numpy as jnp
from jax import lax
from jax.experimental import pallas as pl
from jax.experimental.pallas import tpu as pltpu
from jax.sharding import PartitionSpec as P

MESH = pl.DeviceIdType.MESH
GROUP = 8
SOLVER = 1
SIDE = 0
PASS_FROM = 4
PASS_TO = 2
DOWN = 3
PARTS = 1
TERMS = 4
F32 = jnp.float32
BF16 = jnp.bfloat16


def dot(left, right):
    return jnp.dot(left, right, preferred_element_type=F32)


def kernel(
    n_row, n_col,
    signs_ref, a_ref, b_ref, d_ref,
    out_ref, norm_ref, peak_ref,
    powers, couple, series, strip, solved, below, partial, passed, total, residual,
    stage, peaks, norm_all, peak_all, final_out, next_a,
    total_own, lower, own, partial_out, sign_out, sign_in, final_in, all_a, bounce_near, bounce_far,
    near_send, near_recv, far_send, far_recv, copy_a,
    sign_send, sign_recv, partial_send, partial_recv, below_send, below_recv,
    passed_send, passed_recv, relay_send, own_send, own_recv, extra_send, down_send, up_send, lower_recv,
    skip_send, wrap_send, forward_send, bounce_send, bounce_recv, pass_send, norm_send, norm_recv, peak_send, peak_recv, final_send, final_recv,
):
    r = lax.axis_index("row")
    c = lax.axis_index("col")
    g = c // GROUP
    pos = c % GROUP
    first = g * GROUP
    n_group = n_col // GROUP
    bc = b_ref.shape[1]
    br = d_ref.shape[0]
    wide = GROUP * bc
    half = GROUP // 2
    chunk = br // PARTS
    last_row = n_row - 1
    last_group = n_group - 1
    solver = first + SOLVER
    barrier = pltpu.get_barrier_semaphore()

    def remote(src, dst, send, recv, row, col):
        return pltpu.make_async_remote_copy(
            src_ref=src, dst_ref=dst, send_sem=send, recv_sem=recv,
            device_id=(row, col), device_id_type=MESH,
        )

    def greet(row, col):
        pl.semaphore_signal(barrier, inc=1, device_id=(row, col), device_id_type=MESH)

    def cols(index):
        return pl.ds(pl.multiple_of(index * bc, bc), bc)

    def piece(h):
        return pl.ds(h * chunk, chunk)

    def rows(index, size):
        return pl.ds(pl.multiple_of(index * size, size), size)

    @pl.when(pos == SOLVER)
    def _():
        couple[rows(g, wide), :] = jnp.zeros((wide, wide), BF16)
        for p in range(GROUP):
            if p != SOLVER:
                greet(r, first + p)
        for step in range(1, n_row):
            greet((r + step) % n_row, c)
        for step in range(1, n_group):
            greet(r, (c + step * GROUP) % n_col)

        def fetch():
            return pltpu.make_async_copy(a_ref.at[:, rows(r + 1, br)], next_a, copy_a)

        @pl.when(r < last_row)
        def _():
            fetch().start()

        sign_out[...] = (2 * signs_ref[...] - 1).astype(BF16)
        strip[...] = jnp.zeros(strip.shape, BF16)
        total[...] = jnp.zeros(total.shape, F32)
        peaks[...] = jnp.zeros(peaks.shape, F32)
        for kb in range(SOLVER + 1):
            couple[cols(first + kb), SOLVER * bc:(SOLVER + 1) * bc] = b_ref[cols(first + kb), :]
        for block in range(last_group):
            @pl.when(block < g)
            def _():
                couple[block * wide:(block + 1) * wide, SOLVER * bc:(SOLVER + 1) * bc] = b_ref[block * wide:(block + 1) * wide, :]

        pl.semaphore_wait(barrier, GROUP - 1 + n_row - 1 + n_group - 1)

        def sign_copy():
            return remote(sign_out, sign_in.at[0], sign_send, sign_recv.at[0], r, first + half + 1)

        @pl.when(r < n_row - 2)
        def _():
            sign_copy().start()

        @pl.when(r >= n_row - 2)
        def _():
            partial[SOLVER] = sign_out[...]

        diag = d_ref[...]
        second = dot(diag, diag).astype(BF16)
        powers[:, 0:br] = diag
        powers[:, br:2 * br] = second
        powers[:, 2 * br:3 * br] = dot(second, diag).astype(BF16)
        powers[:, 3 * br:4 * br] = dot(second, second).astype(BF16)

        def pass_on(k):
            return remote(passed.at[k], passed.at[k], relay_send.at[k], passed_recv.at[k], r, (c + GROUP) % n_col)

        for block in range(last_group):
            @pl.when(block < g)
            def _():
                for j in range(GROUP):
                    if j != SOLVER:
                        remote(
                            b_ref.at[pl.ds(block * wide, wide), :],
                            couple.at[pl.ds(block * wide, wide), pl.ds(j * bc, bc)],
                            far_send.at[block], far_recv.at[j, block], r, first + j,
                        ).wait_recv()

                def take(i, carry):
                    k = block * GROUP + i
                    remote(passed.at[k], passed.at[k], relay_send.at[k], passed_recv.at[k], r, (c + n_col - GROUP) % n_col).wait_recv()

                    @pl.when(g < last_group)
                    def _():
                        pass_on(k).start()

                    total[...] -= dot(passed[k], couple[cols(k), :])
                    return carry

                lax.fori_loop(0, GROUP, take, 0)

        @pl.when(r < last_row)
        def _():
            fetch().wait()

        def send_up(j, h):
            return remote(solved.at[j, piece(h)], below.at[j, piece(h)], below_send.at[j, h], below_recv.at[j, h], (r + n_row - 1) % n_row, c)

        def send_right(j):
            return remote(solved.at[j], passed.at[first + j], passed_send.at[j], passed_recv.at[first + j], r, (c + GROUP) % n_col)

        def send_own(j, h):
            return remote(solved.at[j, piece(h)], own.at[1 + j % 2, piece(h)], own_send.at[j, h], own_recv.at[1 + j % 2, h], r, first + j // 2 * 2 + 1)

        def send_side(h):
            return remote(solved.at[SIDE, piece(h)], own.at[0, piece(h)], own_send.at[SIDE, h], own_recv.at[0, h], r, first)

        def send_extra(j, place, h):
            return remote(solved.at[j, piece(h)], own.at[0, piece(h)], extra_send.at[j, h], own_recv.at[0, h], r, first + place)

        def column(j, carry):
            @pl.when(j != SOLVER)
            def _():
                for kb in range(GROUP):
                    @pl.when(kb <= j)
                    def _():
                        remote(
                            b_ref.at[cols(first + kb), :], couple.at[cols(first + kb), cols(j)],
                            near_send.at[kb], near_recv.at[j, kb], r, first + j,
                        ).wait_recv()

            mine = couple[cols(first + j), cols(j)]
            square = dot(mine, mine).astype(BF16)
            series[:, 0:bc] = -mine
            series[:, bc:2 * bc] = square
            series[:, 2 * bc:3 * bc] = (-dot(square, mine)).astype(BF16)
            mid = half * bc
            from_left = pl.multiple_of(g * wide, wide)

            @pl.when(j <= half)
            def _():
                residual[...] = total[:, cols(j)] - dot(strip[:, 0:mid], couple[pl.ds(from_left, mid), cols(j)])

            @pl.when(j > half)
            def _():
                residual[...] = total[:, cols(j)] - dot(strip[...], couple[rows(g, wide), cols(j)])

            @pl.when((j != SOLVER) | (r < n_row - 2))
            def _():
                remote(partial_out.at[1], partial.at[j], partial_send.at[1], partial_recv.at[j], r, first).wait_recv()

            residual[...] += partial[j].astype(F32)

            @pl.when(r < last_row)
            def _():
                for h in range(PARTS):
                    remote(
                        solved.at[j, piece(h)], below.at[j, piece(h)], below_send.at[j, h], below_recv.at[j, h], (r + 1) % n_row, c,
                    ).wait_recv()
                residual[...] -= dot(next_a[...], below[j])

            lead = residual[...].astype(BF16)
            rest = dot(lead, series[...]).astype(BF16)
            stage[0:br, :] = lead
            for m in range(1, TERMS):
                stage[m * br:(m + 1) * br, :] = rest[:, (m - 1) * bc:m * bc]
            for h in range(PARTS):
                solved[j, piece(h), :] = dot(powers[piece(h), :], stage[...]).astype(BF16)

                @pl.when(r > 0)
                def _():
                    send_up(j, h).start()

                @pl.when(r > 1)
                def _():
                    @pl.when(j == SIDE)
                    def _():
                        send_extra(SIDE, half - 1, h).start()

                    @pl.when(j == SOLVER)
                    def _():
                        send_extra(SOLVER, half + 1, h).start()

                @pl.when(j > SOLVER)
                def _():
                    send_own(j, h).start()

                @pl.when(j == SIDE)
                def _():
                    send_side(h).start()

            @pl.when(g < last_group)
            def _():
                send_right(j).start()

            strip[:, cols(j)] = solved[j]
            return carry

        lax.fori_loop(0, GROUP, column, 0)

        def measure(j, carry):
            magnitude = jnp.abs(solved[j].astype(F32))
            peaks[...] = jnp.maximum(peaks[...], magnitude)
            norm_all[r, pl.ds(j, 1), :] = jnp.sum(magnitude, axis=0, keepdims=True)
            return carry

        lax.fori_loop(0, GROUP, measure, 0)

        peak_all[g] = jnp.max(jnp.transpose(peaks[...]), axis=0, keepdims=True)
        for step in range(1, n_row):
            remote(norm_all.at[r], norm_all.at[r], norm_send.at[step - 1], norm_recv.at[r], (r + step) % n_row, c).start()
        for step in range(1, n_group):
            remote(peak_all.at[g], peak_all.at[g], peak_send.at[step - 1], peak_recv.at[g], r, (c + step * GROUP) % n_col).start()
        out_ref[...] = solved[SOLVER]
        for step in range(1, n_row):
            source = (r + step) % n_row
            remote(norm_all.at[source], norm_all.at[source], norm_send.at[step - 1], norm_recv.at[source], source, c).wait_recv()
        for step in range(1, n_group):
            source = (g + step) % n_group
            remote(peak_all.at[source], peak_all.at[source], peak_send.at[step - 1], peak_recv.at[source], r, source * GROUP + SOLVER).wait_recv()
        norms = norm_all[0]
        for source in range(1, n_row):
            norms = norms + norm_all[source]
        top = peak_all[0]
        for source in range(1, n_group):
            top = jnp.maximum(top, peak_all[source])
        for j in range(GROUP):
            final_out[j, :, 0:bc] = norms[j:j + 1, :]
            final_out[j, :, bc:bc + br] = top
        for j in range(GROUP):
            if j != SOLVER:
                remote(final_out.at[j], final_in, final_send.at[j], final_recv, r, first + j).start()
        norm_ref[...] = norms[SOLVER:SOLVER + 1, :]
        peak_ref[...] = top

        @pl.when(r < n_row - 2)
        def _():
            sign_copy().wait_send()

        for block in range(last_group):
            @pl.when((block < g) & (g < last_group))
            def _():
                def drain(i, carry):
                    pass_on(block * GROUP + i).wait_send()
                    return carry

                lax.fori_loop(0, GROUP, drain, 0)

        def finish(j, carry):
            @pl.when(r > 0)
            def _():
                for h in range(PARTS):
                    send_up(j, h).wait_send()

            @pl.when(g < last_group)
            def _():
                send_right(j).wait_send()

            @pl.when(j > SOLVER)
            def _():
                for h in range(PARTS):
                    send_own(j, h).wait_send()

            return carry

        lax.fori_loop(0, GROUP, finish, 0)
        for h in range(PARTS):
            send_side(h).wait_send()

        @pl.when(r > 1)
        def _():
            for h in range(PARTS):
                send_extra(SIDE, half - 1, h).wait_send()
                send_extra(SOLVER, half + 1, h).wait_send()

        for step in range(1, n_row):
            remote(norm_all.at[r], norm_all.at[r], norm_send.at[step - 1], norm_recv.at[r], (r + step) % n_row, c).wait_send()
        for step in range(1, n_group):
            remote(peak_all.at[g], peak_all.at[g], peak_send.at[step - 1], peak_recv.at[g], r, (c + step * GROUP) % n_col).wait_send()
        for j in range(GROUP):
            if j != SOLVER:
                remote(final_out.at[j], final_in, final_send.at[j], final_recv, r, first + j).wait_send()

    def near_copy(kb):
        return remote(
            b_ref.at[cols(first + kb), :], couple.at[cols(first + kb), cols(pos)],
            near_send.at[kb], near_recv.at[pos, kb], r, solver,
        )

    def far_copy(block):
        return remote(
            b_ref.at[pl.ds(block * wide, wide), :],
            couple.at[pl.ds(block * wide, wide), cols(pos)],
            far_send.at[block], far_recv.at[pos, block], r, solver,
        )

    def near_all():
        for kb in range(GROUP):
            @pl.when(kb <= pos)
            def _():
                near_copy(kb).start()

    def far_all():
        for block in range(last_group):
            @pl.when(block < g)
            def _():
                far_copy(block).start()

    def drain_all():
        for kb in range(GROUP):
            @pl.when(kb <= pos)
            def _():
                near_copy(kb).wait_send()
        for block in range(last_group):
            @pl.when(block < g)
            def _():
                far_copy(block).wait_send()

    def close():
        remote(final_in, final_in, final_send.at[0], final_recv, r, solver).wait_recv()
        norm_ref[...] = final_in[:, 0:bc]
        peak_ref[...] = final_in[:, bc:bc + br]

    def give(slot, j):
        return remote(partial_out.at[slot], partial.at[j], partial_send.at[slot], partial_recv.at[j], r, solver)

    def take_own(slot, h):
        remote(own.at[slot, piece(h)], own.at[slot, piece(h)], skip_send.at[0, h], own_recv.at[slot, h], r, solver).wait_recv()

    @pl.when(pos % 2 == 0)
    def _():
        greet(r, solver)

        @pl.when(pos == 0)
        def _():
            greet(r, first + half - 1)

        @pl.when(pos > 0)
        def _():
            greet(r, c + 1)

        @pl.when(pos == PASS_FROM)
        def _():
            greet(r, first + PASS_TO)

        @pl.when(pos == PASS_TO)
        def _():
            greet(r, first + PASS_FROM)

        partial_out[1] = (2 * signs_ref[...] - 1).astype(BF16)

        @pl.when((pos == PASS_FROM) | (pos == PASS_TO))
        def _():
            pl.semaphore_wait(barrier, 3)

        @pl.when((pos != PASS_FROM) & (pos != PASS_TO))
        def _():
            pl.semaphore_wait(barrier, 2)

        def sign_zero():
            return remote(partial_out.at[1], sign_in.at[0], sign_send, sign_recv.at[0], r, first + half - 1)

        def sign_next():
            return remote(partial_out.at[1], sign_in.at[1], sign_send, sign_recv.at[1], r, c + 1)

        def lend_near():
            return remote(b_ref.at[rows(g, wide), :], bounce_near, near_send.at[0], bounce_recv.at[n_group], r, first + PASS_TO)

        def lend_far(block):
            return remote(b_ref.at[pl.ds(block * wide, wide), :], bounce_far.at[block], far_send.at[block], bounce_recv.at[block], r, first + PASS_TO)

        def pass_near(kb):
            return remote(
                bounce_near.at[pl.ds(kb * bc, bc), :], couple.at[cols(first + kb), pl.ds(PASS_FROM * bc, bc)],
                bounce_send.at[kb], near_recv.at[PASS_FROM, kb], r, solver,
            )

        def pass_far(block):
            return remote(
                bounce_far.at[block], couple.at[pl.ds(block * wide, wide), pl.ds(PASS_FROM * bc, bc)],
                pass_send.at[block], far_recv.at[PASS_FROM, block], r, solver,
            )

        @pl.when((r < n_row - 2) & (pos == 0))
        def _():
            sign_zero().start()

        @pl.when((r < n_row - 2) & (pos > 0))
        def _():
            sign_next().start()

        @pl.when(pos != PASS_FROM)
        def _():
            far_all()

        for block in range(last_group):
            @pl.when((pos == PASS_FROM) & (block < g))
            def _():
                lend_far(block).start()

            @pl.when((pos == PASS_TO) & (block < g))
            def _():
                lend_far(block).wait_recv()
                pass_far(block).start()

        @pl.when(pos == PASS_FROM)
        def _():
            lend_near().start()

        @pl.when(pos != PASS_FROM)
        def _():
            near_all()

        @pl.when(r >= n_row - 2)
        def _():
            give(1, pos).start()

        @pl.when(pos == PASS_TO)
        def _():
            lend_near().wait_recv()
            for kb in range(PASS_FROM + 1):
                pass_near(kb).start()

        for h in range(PARTS):
            take_own(0, h)
        out_ref[...] = own[0]

        @pl.when(r < n_row - 2)
        def _():
            sign_next().wait_send()

        @pl.when(r >= n_row - 2)
        def _():
            give(1, pos).wait_send()

        @pl.when(pos == PASS_FROM)
        def _():
            lend_near().wait_send()
            for block in range(last_group):
                @pl.when(block < g)
                def _():
                    lend_far(block).wait_send()

        @pl.when(pos == PASS_TO)
        def _():
            for kb in range(PASS_FROM + 1):
                pass_near(kb).wait_send()
            for block in range(last_group):
                @pl.when(block < g)
                def _():
                    pass_far(block).wait_send()

        @pl.when(pos != PASS_FROM)
        def _():
            drain_all()

        close()

    @pl.when((pos % 2 == 1) & (pos > SOLVER))
    def _():
        extra = pos // 2 - 1
        has_extra = pos < GROUP - 1

        def fetch():
            return pltpu.make_async_copy(a_ref, all_a, copy_a)

        greet(r, solver)
        greet(r, c - 1)
        for step in range(1, n_row):
            greet((r + step) % n_row, c)

        @pl.when(pos == half - 1)
        def _():
            greet(r, first)

        fetch().start()
        signs = 2 * signs_ref[...] - 1
        total_own[2] = signs.astype(F32)
        partial_out[2] = signs.astype(BF16)

        @pl.when(pos == half - 1)
        def _():
            pl.semaphore_wait(barrier, n_row + 2)

        @pl.when(pos != half - 1)
        def _():
            pl.semaphore_wait(barrier, n_row + 1)

        far_all()
        near_all()

        @pl.when(r >= n_row - 2)
        def _():
            give(2, pos).start()


        @pl.when(r < n_row - 2)
        def _():
            remote(sign_in.at[1], sign_in.at[1], sign_send, sign_recv.at[1], r, c - 1).wait_recv()
            total_own[1] = sign_in[1].astype(F32)

            @pl.when(has_extra)
            def _():
                remote(sign_in.at[0], sign_in.at[0], sign_send, sign_recv.at[0], r, solver).wait_recv()
                total_own[0] = sign_in[0].astype(F32)

        fetch().wait()

        def lower_copy(slot, k, sems, row, h):
            return remote(lower.at[slot, k, piece(h)], lower.at[slot, k, piece(h)], sems.at[slot, k, h], lower_recv.at[slot, k, h], row, c)

        def relay_down(slot, k, h):
            return lower_copy(slot, k, down_send, (r + n_row - 1) % n_row, h)

        def relay_up(slot, k, h):
            return lower_copy(slot, k, up_send, (r + 1) % n_row, h)

        def skip(slot, h):
            return remote(own.at[slot, piece(h)], lower.at[slot, r, piece(h)], skip_send.at[slot, h], lower_recv.at[slot, r, h], (r + n_row - 2) % n_row, c)

        def wrap(slot, h):
            return remote(own.at[slot, piece(h)], lower.at[slot, r, piece(h)], wrap_send.at[slot, h], lower_recv.at[slot, r, h], 0, c)

        def forward(h):
            return remote(own.at[1, piece(h)], own.at[0, piece(h)], forward_send.at[h], own_recv.at[0, h], r, c - 1)

        def goes_down(k):
            return (k >= r + 2) & (k < r + DOWN) & (r > 0)

        def apply(slot, k):
            for h in range(PARTS):
                lower_copy(slot, k, down_send, (r + 1) % n_row, h).wait_recv()

                @pl.when(goes_down(k))
                def _():
                    relay_down(slot, k, h).start()

                @pl.when(k >= r + DOWN + 2)
                def _():
                    relay_up(slot, k, h).start()

            total_own[slot] -= dot(all_a[:, rows(k, br)], lower[slot, k])

        def handle(slot, k, j):
            @pl.when((k >= r + 2) & (k <= last_row))
            def _():
                apply(slot, k)

                @pl.when(k == r + 2)
                def _():
                    partial_out[slot] = total_own[slot].astype(BF16)
                    give(slot, j).start()

        def spread(slot):
            for h in range(PARTS):
                take_own(slot, h)

                @pl.when(r > 1)
                def _():
                    skip(slot, h).start()

                @pl.when(r > DOWN)
                def _():
                    wrap(slot, h).start()

        def event(i, carry):
            early = last_row - i
            late = last_row - i + 1

            @pl.when(has_extra)
            def _():
                handle(0, early, extra)

                @pl.when((early == r) & (r > 1))
                def _():
                    spread(0)

            handle(1, late, pos - 1)

            @pl.when(late == r)
            def _():
                spread(1)
                for h in range(PARTS):
                    forward(h).start()

            handle(2, late, pos)

            @pl.when(late == r)
            def _():
                spread(2)

            return carry

        lax.fori_loop(0, n_row + 2, event, 0)
        out_ref[...] = own[2]
        for h in range(PARTS):
            forward(h).wait_send()
        give(2, pos).wait_send()

        @pl.when(r < n_row - 2)
        def _():
            give(1, pos - 1).wait_send()

            @pl.when(has_extra)
            def _():
                give(0, extra).wait_send()

        def settle_slot(slot):
            def settle(i, carry):
                k = last_row - i

                @pl.when(goes_down(k))
                def _():
                    for h in range(PARTS):
                        relay_down(slot, k, h).wait_send()

                @pl.when(k >= r + DOWN + 2)
                def _():
                    for h in range(PARTS):
                        relay_up(slot, k, h).wait_send()

                return carry

            lax.fori_loop(0, n_row - 2, settle, 0)

            @pl.when(r > 1)
            def _():
                for h in range(PARTS):
                    skip(slot, h).wait_send()

            @pl.when(r > DOWN)
            def _():
                for h in range(PARTS):
                    wrap(slot, h).wait_send()

        @pl.when(has_extra)
        def _():
            settle_slot(0)

        settle_slot(1)
        settle_slot(2)
        drain_all()
        close()


def hand_out(solved_ref, norm_ref, peak_ref, solved_out, norm_out, peak_out):
    solved_out[...] = solved_ref[...]
    norm_out[...] = norm_ref[...]
    peak_out[...] = peak_ref[...]


def solution(mesh):
    n_row = mesh.shape["row"]
    n_col = mesh.shape["col"]

    def shards(signs, upper_a, upper_b, diag_inverse):
        br = diag_inverse.shape[0]
        bc = upper_b.shape[1]
        order = upper_b.shape[0]
        wide = GROUP * bc
        n_group = n_col // GROUP
        dma = pltpu.SemaphoreType.DMA
        vmem = pl.BlockSpec(memory_space=pltpu.VMEM)
        shapes = (
            jax.ShapeDtypeStruct((br, bc), BF16),
            jax.ShapeDtypeStruct((1, bc), F32),
            jax.ShapeDtypeStruct((1, br), F32),
        )
        results = pl.pallas_call(
            functools.partial(kernel, n_row, n_col),
            out_shape=shapes,
            in_specs=[vmem, pl.BlockSpec(memory_space=pl.ANY), vmem, vmem],
            out_specs=[vmem] * 3,
            scratch_shapes=[
                pltpu.VMEM((br, TERMS * br), BF16),
                pltpu.VMEM((order, wide), BF16),
                pltpu.VMEM((bc, (TERMS - 1) * bc), BF16),
                pltpu.VMEM((br, wide), BF16),
                pltpu.VMEM((GROUP, br, bc), BF16),
                pltpu.VMEM((GROUP, br, bc), BF16),
                pltpu.VMEM((GROUP, br, bc), BF16),
                pltpu.VMEM((n_col, br, bc), BF16),
                pltpu.VMEM((br, wide), F32),
                pltpu.VMEM((br, bc), F32),
                pltpu.VMEM((TERMS * br, bc), BF16),
                pltpu.VMEM((br, bc), F32),
                pltpu.VMEM((n_row, GROUP, bc), F32),
                pltpu.VMEM((n_group, 1, br), F32),
                pltpu.VMEM((GROUP, 1, bc + br), F32),
                pltpu.VMEM((br, br), BF16),
                pltpu.VMEM((3, br, bc), F32),
                pltpu.VMEM((3, n_row, br, bc), BF16),
                pltpu.VMEM((3, br, bc), BF16),
                pltpu.VMEM((3, br, bc), BF16),
                pltpu.VMEM((br, bc), BF16),
                pltpu.VMEM((2, br, bc), BF16),
                pltpu.VMEM((1, bc + br), F32),
                pltpu.VMEM((br, n_row * br), BF16),
                pltpu.VMEM((wide, bc), BF16),
                pltpu.VMEM((n_group, wide, bc), BF16),
                dma((GROUP,)), dma((GROUP, GROUP)),
                dma((n_group,)), dma((GROUP, n_group)),
                dma,
                dma, dma((2,)),
                dma((3,)), dma((GROUP,)),
                dma((GROUP, PARTS)), dma((GROUP, PARTS)),
                dma((GROUP,)), dma((n_col,)),
                dma((n_col,)),
                dma((GROUP, PARTS)), dma((3, PARTS)),
                dma((2, PARTS)),
                dma((3, n_row, PARTS)), dma((3, n_row, PARTS)), dma((3, n_row, PARTS)),
                dma((3, PARTS)), dma((3, PARTS)), dma((PARTS,)),
                dma((GROUP,)), dma((n_group + 1,)), dma((n_group,)),
                dma((n_row,)), dma((n_row,)),
                dma((n_group,)), dma((n_group,)),
                dma((GROUP,)), dma,
            ],
            compiler_params=pltpu.CompilerParams(
                collective_id=0, has_side_effects=True, vmem_limit_bytes=60 * 1024 * 1024
            ),
        )(signs[0], upper_a, upper_b, diag_inverse)
        solved, norms, peaks = pl.pallas_call(
            hand_out, out_shape=shapes, in_specs=[vmem] * 3, out_specs=[vmem] * 3
        )(*results)
        return solved[None], norms, peaks

    in_specs = (P(None, "row", "col"), P("row", None), P(None, "col"), P("row", None))
    out_specs = (P(None, "row", "col"), P(None, "col"), P(None, "row"))
    return jax.shard_map(shards, mesh=mesh, in_specs=in_specs, out_specs=out_specs, check_vma=False)
```
